32 devices in a mesh: bunch: 8 (over z, x), dom: 4 (over y, core).
Axes of the slice: x: 2, y: 2, z: 4, core: 2. Of those that a mesh axis runs over, the one named last changes fastest.
Arguments:
- positions: float32 [2, 2, 16, 4096], P(None, None, 'bunch', 'dom'), may hold values from 0 to 127
- momenta: float32 [2, 2, 16, 4096], P(None, None, 'bunch', 'dom'), may hold values from -6 to 6
- kernel_hat: float32 [2, 2, 256, 256], replicated, may hold values from -1.2 to 1.2
- partners: int32 [2, 16, 16], P(None, 'bunch'), may hold values from 0 to 15, as said below
- offsets: int32 [2, 2, 16, 16], P(None, None, 'bunch'), may hold values from -32 to 32
- counts: int32 [2, 16], P(None, 'bunch'), may hold values from 1 to 16, as said below
Outputs:
- kicked: float32 [2, 2, 16, 4096], P(None, None, 'bunch', 'dom')
The draws below stay inside these ranges and needn't reach their ends.
Inputs may be any that keep to these rules, and one draw needn't show every extreme that they name: partners[e, b, s] // 2 lies at most 2 from b // 2, counted around a cycle of 8 blocks. `counts`: the first bunch of each block of 2 bunches has all 16 slots live.
All inputs are finite; a program needn't handle non-finite values.
Results may differ from the reference program's by a relative error of at most 0.0003.
Values sent between devices are 32-bit elements; how exact they have to be, the bound alone decides.
A program may use at most 64 MiB of HBM per device.

```python
import jax
import jax.numpy as jnp
from jax import lax

GRID = 128
PAD = 256
BPB = 2
SLOTS = 16
HOPS = 2
OFFSET = 32
NB = 16
PART = 4096


def draw_partners(key, part):
    key_block = jax.random.fold_in(key, 11)
    key_member = jax.random.fold_in(key, 12)
    blocks = NB // BPB
    home = (jnp.arange(NB, dtype=jnp.int32) // BPB)[None, :, None]
    jumps = jax.random.randint(key_block, (2, NB, SLOTS), 0 - HOPS, HOPS + 1)
    member = jax.random.randint(key_member, (2, NB, SLOTS), 0, BPB)
    return ((home + jumps) % blocks * BPB + member).astype(jnp.int32)


def draw_counts(key, part):
    key_count = jax.random.fold_in(key, 21)
    drawn = jax.random.randint(key_count, (2, NB), 1, SLOTS + 1)
    first = (jnp.arange(NB, dtype=jnp.int32) % BPB == 0)[None, :]
    return jnp.where(first, SLOTS, drawn).astype(jnp.int32)


def touch_ends(array, key, low, largest):
    dims = array.shape
    place = [jax.random.randint(jax.random.fold_in(key, axis), (), 0, dims[axis]) for axis in range(len(dims))]
    array = array.at[tuple(place)].set(low)
    longest = dims.index(max(dims))
    place[longest] = (place[longest] + 1) % dims[longest]
    return array.at[tuple(place)].set(largest)


def levels(stream_key, extent, cuts, low, high):
    gain = 1.0
    for dim, parts in cuts:
        steps = jax.random.uniform(jax.random.fold_in(jax.random.fold_in(stream_key, 6), dim), (parts,), jnp.float32, low / len(cuts), high / len(cuts))
        gain = gain * jnp.repeat(jnp.exp(steps), extent[dim] // parts).reshape((-1,) + (1,) * (len(extent) - 1 - dim))
    return gain


def centred(key, dims, deviation, reach, pieces=(), kind=jnp.bfloat16):
    entries = deviation * jax.random.normal(key, dims, jnp.float32)
    if pieces:
        entries = entries * levels(key, dims, pieces, -0.22, 0.18)
    return jnp.clip(entries, -reach, reach).astype(kind)


def setup_inputs(seed: int = 0) -> dict:
    arg_keys = jax.random.split(jax.random.key(seed), 7)
    positions = jnp.clip(127.0 * jax.random.uniform(arg_keys[0], (2, 2, NB, PART), jnp.float32) ** levels(arg_keys[0], (2, 2, NB, PART), ((2, 8), (3, 4)), -0.2, 0.2), 0.0, 127.0)
    momenta = centred(arg_keys[1], (2, 2, NB, PART), 1.0, 6.0, ((2, 8), (3, 4)), jnp.float32)
    kernel_hat = centred(arg_keys[2], (2, 2, PAD, PAD), 0.2, 1.2, (), jnp.float32)
    partners = draw_partners(jax.random.fold_in(arg_keys[6], 71), 0)
    offsets = touch_ends(jax.random.randint(arg_keys[4], (2, 2, NB, SLOTS), 0 - OFFSET, OFFSET + 1), jax.random.fold_in(arg_keys[4], 1), 0 - OFFSET, OFFSET).astype(jnp.int32)
    counts = draw_counts(jax.random.fold_in(arg_keys[6], 71), 0)
    return dict(positions=positions, momenta=momenta, kernel_hat=kernel_hat, partners=partners, offsets=offsets, counts=counts)


HIGH = lax.Precision.HIGHEST


def hat_table(coord):
    cells = jnp.arange(GRID, dtype=jnp.float32)
    return jnp.maximum(0.0, 1.0 - jnp.abs(coord[:, None] - cells[None, :]))


def deposit(coords):
    weight_x = hat_table(coords[0])
    weight_y = hat_table(coords[1])
    return jnp.dot(weight_x.T, weight_y, precision=HIGH, preferred_element_type=jnp.float32)


def kick(coords, fields, moments):
    weight_x = hat_table(coords[0])
    weight_y = hat_table(coords[1])
    field_x = jnp.sum(jnp.dot(weight_x, fields[0], precision=HIGH, preferred_element_type=jnp.float32) * weight_y, axis=1)
    field_y = jnp.sum(jnp.dot(weight_x, fields[1], precision=HIGH, preferred_element_type=jnp.float32) * weight_y, axis=1)
    return moments + jnp.stack([field_x, field_y])


def reference(positions, momenta, kernel_hat, partners, offsets, counts):
    coords = jnp.transpose(positions.reshape(2, 2 * NB, PART), (1, 0, 2))
    grids = lax.map(deposit, coords)

    def field_of(target):
        beam = target // NB
        bunch = target % NB
        row = partners[beam, bunch]
        shift_x = offsets[0, beam, bunch]
        shift_y = offsets[1, beam, bunch]
        live_count = counts[beam, bunch]

        def add_one(slot, total):
            index = ((1 - beam) * NB + row[slot]).astype(jnp.int32)
            grid = lax.dynamic_index_in_dim(grids, index, 0, keepdims=False)
            padded = jnp.pad(grid, ((0, PAD - GRID), (0, PAD - GRID)))
            moved = jnp.roll(padded, (shift_x[slot], shift_y[slot]), axis=(0, 1))
            live = (slot < live_count).astype(jnp.float32)
            return total + live * moved

        summed = lax.fori_loop(0, SLOTS, add_one, jnp.zeros((PAD, PAD), jnp.float32))
        spectrum = jnp.fft.fft2(summed)
        kernel = kernel_hat[:, 0] + 1j * kernel_hat[:, 1]
        return jnp.real(jnp.fft.ifft2(kernel * spectrum[None]))[:, :GRID, :GRID]

    fields = lax.map(field_of, jnp.arange(2 * NB, dtype=jnp.int32))
    moments = jnp.transpose(momenta.reshape(2, 2 * NB, PART), (1, 0, 2))
    kicked = lax.map(lambda item: kick(item[0], item[1], item[2]), (coords, fields, moments))
    return jnp.transpose(kicked, (1, 0, 2)).reshape(2, 2, NB, PART)
```

```python
import functools

import jax
import jax.numpy as jnp
import ml_dtypes
import numpy as np
from jax import lax
from jax.experimental import pallas as pl
from jax.experimental.pallas import tpu as pltpu
from jax.sharding import PartitionSpec as P

HOPS = 2
OFFSET = 32
LANES = 256
MESH = pl.DeviceIdType.MESH
BF = jnp.bfloat16
F32 = jnp.float32


def split(x):
    high = x.astype(BF)
    return high, (x - high.astype(F32)).astype(BF)


def dot(a, b):
    return jnp.dot(a, b, preferred_element_type=F32)


def dot3(ah, al, bh, bl):
    return dot(ah, bh) + dot(ah, bl) + dot(al, bh)


def hat(row, cells):
    centres = lax.broadcasted_iota(jnp.int32, (cells, row.shape[1]), 0).astype(F32)
    return jnp.maximum(0.0, 1.0 - jnp.abs(row - centres))


def np_split(table):
    table = table.astype(np.float32)
    high = table.astype(ml_dtypes.bfloat16)
    low = (table - high.astype(np.float32)).astype(ml_dtypes.bfloat16)
    return np.stack([high, low])


def dft_tables(padded, cells, rows):
    k = np.arange(padded)

    def cs(left, right):
        angle = 2.0 * np.pi * (np.outer(left, right) % padded) / padded
        return np.cos(angle), np.sin(angle)

    c1, s1 = cs(k, np.arange(rows) - OFFSET)
    c2, s2 = cs(k, k)
    c3, s3 = cs(k, np.arange(cells))
    c4, s4 = cs(np.arange(cells), k)
    t1 = np.concatenate([c1, -s1], 0)
    t2 = np.concatenate([c2, s2], 0)
    t3 = np.block([[c3, s3], [-s3, c3]])
    t4 = np.concatenate([c4, -s4], 1) / float(padded * padded)
    return [np_split(t) for t in (t1, t2, t3, t4)]


def body(
    nb, nd, bpb, cells, padded, parts, slots,
    partners, offsets, counts, pos, mom, kernel_hbm, t1_hbm, t2_hbm, t3_hbm, t4_hbm,
    out,
    pos_s, rx, tx, ty, win, wx, wy, src, res, fin, kern, t1, t2, t3, t4,
    pos_send, pos_recv, win_send, win_recv, mate_send, mate_recv, res_send, res_recv, load_sem,
):
    local = 2 * bpb
    b = lax.axis_index("bunch")
    d = lax.axis_index("dom")
    beam = lax.div(d, bpb)
    member = lax.rem(d, bpb)
    source = lax.rem(d + bpb, local)
    pad = 2 * OFFSET
    rows = cells + pad

    def at(block, dom):
        return (block, dom)

    barrier = pltpu.get_barrier_semaphore()
    jumps = [j for h in range(1, HOPS + 1) for j in (h, -h)]
    for k in range(1, nd):
        pl.semaphore_signal(barrier, inc=1, device_id=at(b, lax.rem(d + k, nd)), device_id_type=MESH)
    for j in jumps:
        pl.semaphore_signal(barrier, inc=1, device_id=at(lax.rem(b + j + nb, nb), d), device_id_type=MESH)

    loads = [
        pltpu.make_async_copy(a, v, load_sem.at[i])
        for i, (a, v) in enumerate(
            [(t1_hbm, t1), (t2_hbm, t2), (kernel_hbm, kern), (t3_hbm, t3), (t4_hbm, t4)]
        )
    ]
    for load in loads:
        load.start()
    for e in range(2):
        for m in range(bpb):
            for c in range(2):
                pos_s[e * bpb + m, c : c + 1, :] = pos[c, e, m : m + 1, :]
    zero = jnp.zeros((2 * HOPS + 1, bpb, pad, cells), F32)
    win[:, :, :pad, :] = zero
    win[:, :, pad + cells :, :] = zero
    pl.semaphore_wait(barrier, nd - 1 + len(jumps))

    sends = []
    for which in range(2):
        for k in range(1, nd):
            peer = lax.rem(d + k, nd)
            bunch = lax.rem(peer + bpb, local) if which == 0 else peer
            copy = pltpu.make_async_remote_copy(
                src_ref=pos_s.at[bunch],
                dst_ref=rx.at[k - 1, which],
                send_sem=pos_send.at[k - 1, which],
                recv_sem=pos_recv.at[k - 1, which],
                device_id=at(b, peer),
                device_id_type=MESH,
            )
            copy.start()
            sends.append(copy)

    def fill(coords):
        for p in range(0, parts, LANES):
            sl = slice(p, p + LANES)
            high, low = split(hat(coords[0:1, sl], cells))
            tx[:cells, sl] = high
            tx[cells:, sl] = low
            high, low = split(hat(coords[1:2, sl], cells))
            ty[:cells, sl] = high
            ty[cells:, sl] = low
        return lax.dot_general(
            tx[...], ty[...], (((1,), (1,)), ((), ())), preferred_element_type=F32
        )

    total = fill(pos_s[source])
    for k in range(1, nd):
        sends[k - 1].wait_recv()
        total = total + fill(rx[k - 1, 0])
    grid = (
        total[:cells, :cells] + total[:cells, cells:] + total[cells:, :cells] + total[cells:, cells:]
    )
    band = pl.ds(pad, cells)
    win[HOPS, member, band, :] = grid

    grid_sends = {}
    for i, j in enumerate(jumps):
        copy = pltpu.make_async_remote_copy(
            src_ref=win.at[HOPS, member, band],
            dst_ref=win.at[HOPS - j, member, band],
            send_sem=win_send.at[i],
            recv_sem=win_recv.at[i],
            device_id=at(lax.rem(b + j + nb, nb), d),
            device_id_type=MESH,
        )
        copy.start()
        grid_sends[j] = copy
    mate_sends = []

    def to_mates(place):
        for k in range(1, bpb):
            mate = beam * bpb + lax.rem(member + k, bpb)
            copy = pltpu.make_async_remote_copy(
                src_ref=win.at[place, member, band],
                dst_ref=win.at[place, member, band],
                send_sem=mate_send.at[place, k - 1],
                recv_sem=mate_recv.at[place, k - 1],
                device_id=at(b, mate),
                device_id_type=MESH,
            )
            copy.start()
            mate_sends.append((place, k, copy))

    to_mates(HOPS)

    def kick_tables(coords, base):
        for p in range(0, parts, LANES):
            sl = slice(p, p + LANES)
            to = slice(base + p, base + p + LANES)
            wx[:, to] = hat(coords[0:1, sl], cells)
            high, low = split(hat(coords[1:2, sl], cells))
            wy[:cells, to] = high
            wy[cells : 2 * cells, to] = high
            wy[2 * cells :, to] = low

    kick_tables(pos_s[d], 0)
    for k in range(1, nd):
        sends[nd - 1 + k - 1].wait_recv()
        kick_tables(rx[k - 1, 1], k * parts)

    for j in jumps:
        grid_sends[j].wait_recv()
        to_mates(HOPS - j)
    for place, k, copy in mate_sends:
        copy.wait_recv()

    live_count = counts[beam, member]
    lane = lax.broadcasted_iota(jnp.int32, (8, cells), 1)
    chosen = []
    for s in range(slots):
        row = partners[beam, member, s]
        place = jnp.minimum(lax.rem(lax.div(row, bpb) - b + HOPS + nb, nb), 2 * HOPS)
        shift_x = offsets[0, beam, member, s]
        shift_y = offsets[1, beam, member, s]
        turn = jnp.where(shift_y < 0, shift_y + cells, shift_y)
        live = jnp.where(s < live_count, 1.0, 0.0).astype(F32)
        wrap = jnp.where(shift_y < 0, 1, 0)
        upper = jnp.where(lane >= turn, 1, 0)
        first = jnp.where(upper != wrap, live, 0.0)
        chosen.append((place, lax.rem(row, bpb), OFFSET - shift_x, turn, first, live - first))
    step = 2 * OFFSET
    for r in range(0, rows, step):
        low_half = jnp.zeros((step, cells), F32)
        high_half = jnp.zeros((step, cells), F32)
        for place, which, start, turn, first, second in chosen:
            piece = win[place, which, pl.ds(start + r, step), :]
            piece = pltpu.roll(piece, turn, 1)
            low_half = low_half + piece * jnp.concatenate([first] * (step // 8), 0)
            high_half = high_half + piece * jnp.concatenate([second] * (step // 8), 0)
        src[r : r + step, :cells] = low_half
        src[r : r + step, cells:] = high_half

    loads[0].wait()
    sh, sl = split(src[...])
    spec = dot3(t1[0], t1[1], sh, sl)
    real, imag = spec[:padded], spec[padded:]
    ah, al = split(real)
    bh, bl = split(imag)

    def pair(x, y):
        return jnp.concatenate(
            [jnp.concatenate([x, y], 1), jnp.concatenate([y, -x], 1)], 0
        )

    loads[1].wait()
    spec = dot3(pair(ah, bh), pair(al, bl), t2[0], t2[1])
    real, imag = spec[:padded], spec[padded:]
    loads[2].wait()
    mixed = []
    for c in range(2):
        kr, ki = kern[c, 0], kern[c, 1]
        mixed.append(jnp.concatenate([kr * real - ki * imag, kr * imag + ki * real], 1))
    mh, ml = split(jnp.concatenate(mixed, 0))
    loads[3].wait()
    half = dot3(mh, ml, t3[0], t3[1])
    g0, g1 = half[:padded], half[padded:]
    stacked = jnp.concatenate(
        [
            jnp.concatenate([g0[:, :cells], g1[:, :cells]], 1),
            jnp.concatenate([g0[:, cells:], g1[:, cells:]], 1),
        ],
        0,
    )
    gh, gl = split(stacked)
    loads[4].wait()
    field = dot3(t4[0], t4[1], gh, gl)
    fh, fl = split(jnp.concatenate([field[:, :cells], field[:, cells:]], 0))
    weights = jnp.concatenate([fh, fl, fh], 1)

    def kicks(k):
        for p in range(0, parts, LANES):
            sl = slice(k * parts + p, k * parts + p + LANES)
            z = dot(weights, wy[:, sl])
            w = wx[:, sl]
            for c in range(2):
                row = jnp.sum(z[c * cells : (c + 1) * cells] * w, axis=0, keepdims=True)
                res[k, c : c + 1, p : p + LANES] = row

    res_sends = []
    for k in range(1, nd):
        kicks(k)
        copy = pltpu.make_async_remote_copy(
            src_ref=res.at[k],
            dst_ref=fin.at[d],
            send_sem=res_send.at[k - 1],
            recv_sem=res_recv.at[k - 1],
            device_id=at(b, lax.rem(d - k + nd, nd)),
            device_id_type=MESH,
        )
        copy.start()
        res_sends.append(copy)
    kicks(0)
    fin[d] = res[0]
    for copy in res_sends:
        copy.wait_recv()
    for e in range(2):
        for m in range(bpb):
            for c in range(2):
                out[c, e, m : m + 1, :] = mom[c, e, m : m + 1, :] + fin[e * bpb + m, c : c + 1, :]
    for copy in sends + list(grid_sends.values()) + res_sends:
        copy.wait_send()
    for _, _, copy in mate_sends:
        copy.wait_send()


def solution(mesh):
    nb, nd = mesh.shape["bunch"], mesh.shape["dom"]

    def per_device(positions, momenta, kernel_hat, partners, offsets, counts):
        bpb = positions.shape[2]
        parts = positions.shape[3]
        padded = kernel_hat.shape[-1]
        cells = padded // 2
        slots = partners.shape[-1]
        local = 2 * bpb
        assert local == nd and nb > 2 * HOPS
        pad = 2 * OFFSET
        rows = cells + pad
        tables = [jnp.asarray(t) for t in dft_tables(padded, cells, rows)]
        vmem = pl.BlockSpec(memory_space=pltpu.VMEM)
        smem = pl.BlockSpec(memory_space=pltpu.SMEM)
        anym = pl.BlockSpec(memory_space=pl.ANY)
        dma = pltpu.SemaphoreType.DMA
        return pl.pallas_call(
            functools.partial(body, nb, nd, bpb, cells, padded, parts, slots),
            out_shape=jax.ShapeDtypeStruct(momenta.shape, F32),
            in_specs=[smem] * 3 + [vmem] * 2 + [anym] * 5,
            out_specs=vmem,
            scratch_shapes=[
                pltpu.VMEM((local, 2, parts), F32),
                pltpu.VMEM((nd - 1, 2, 2, parts), F32),
                pltpu.VMEM((2 * cells, parts), BF),
                pltpu.VMEM((2 * cells, parts), BF),
                pltpu.VMEM((2 * HOPS + 1, bpb, cells + 2 * pad, cells), F32),
                pltpu.VMEM((cells, nd * parts), F32),
                pltpu.VMEM((3 * cells, nd * parts), BF),
                pltpu.VMEM((rows, padded), F32),
                pltpu.VMEM((nd, 2, parts), F32),
                pltpu.VMEM((local, 2, parts), F32),
                pltpu.VMEM(kernel_hat.shape, F32),
            ]
            + [pltpu.VMEM(t.shape, BF) for t in tables]
            + [
                dma((nd - 1, 2)),
                dma((nd - 1, 2)),
                dma((2 * HOPS,)),
                dma((2 * HOPS,)),
                dma((2 * HOPS + 1, bpb - 1)),
                dma((2 * HOPS + 1, bpb - 1)),
                dma((nd - 1,)),
                dma((nd - 1,)),
                dma((5,)),
            ],
            compiler_params=pltpu.CompilerParams(collective_id=0, has_side_effects=True),
            name="beam_kick",
        )(partners, offsets, counts, positions, momenta, kernel_hat, *tables)

    spec = P(None, None, "bunch", "dom")
    return jax.shard_map(
        per_device,
        mesh=mesh,
        in_specs=(spec, spec, P(), P(None, "bunch", None), P(None, None, "bunch", None), P(None, "bunch")),
        out_specs=spec,
        check_vma=False,
    )
```

```python
import functools

import jax
import jax.numpy as jnp
import ml_dtypes
import numpy as np
from jax import lax
from jax.experimental import pallas as pl
from jax.experimental.pallas import tpu as pltpu
from jax.sharding import PartitionSpec as P

HOPS = 2
OFFSET = 32
LANES = 256
MESH = pl.DeviceIdType.MESH
BF = jnp.bfloat16
F32 = jnp.float32


def split(x):
    high = x.astype(BF)
    return high, (x - high.astype(F32)).astype(BF)


def dot(a, b):
    return jnp.dot(a, b, preferred_element_type=F32)


def dot3(ah, al, bh, bl):
    return dot(ah, bh) + dot(ah, bl) + dot(al, bh)


def hat(row, cells):
    centres = lax.broadcasted_iota(jnp.int32, (cells, row.shape[1]), 0).astype(F32)
    return jnp.maximum(0.0, 1.0 - jnp.abs(row - centres))


def hat_split(row, cells):
    below = jnp.floor(row)
    above = below + 1.0
    h0, l0 = split(1.0 - jnp.abs(row - below))
    h1, l1 = split(1.0 - jnp.abs(row - above))
    centres = lax.broadcasted_iota(jnp.int32, (cells, row.shape[1]), 0).astype(F32).astype(BF)
    at0 = centres == below.astype(BF)
    at1 = centres == above.astype(BF)
    none = jnp.zeros((), BF)
    return jnp.where(at0, h0, jnp.where(at1, h1, none)), jnp.where(at0, l0, jnp.where(at1, l1, none))


def np_split(table):
    table = table.astype(np.float32)
    high = table.astype(ml_dtypes.bfloat16)
    low = (table - high.astype(np.float32)).astype(ml_dtypes.bfloat16)
    return np.stack([high, low])


def dft_tables(padded, cells, rows):
    k = np.arange(padded)

    def cs(left, right):
        angle = 2.0 * np.pi * (np.outer(left, right) % padded) / padded
        return np.cos(angle), np.sin(angle)

    c1, s1 = cs(k, np.arange(rows) - OFFSET)
    c2, s2 = cs(k, k)
    c3, s3 = cs(k, np.arange(cells))
    c4, s4 = cs(np.arange(cells), k)
    t1 = np.concatenate([c1, -s1], 0)
    t2 = np.concatenate([c2, s2], 0)
    t3 = np.block([[c3, s3], [-s3, c3]])
    t4 = np.concatenate([c4, -s4], 1) / float(padded * padded)
    return [np_split(t) for t in (t1, t2, t3, t4)]


def body(
    nb, nd, bpb, cells, padded, parts, slots,
    partners, offsets, counts, pos, kernel_hbm, t1_hbm, t2_hbm, t3_hbm, t4_hbm,
    out,
    pos_s, rx, tx, ty, win, wx, wy, src, res, fin, kern, t1, t2, t3, t4,
    pos_send, pos_recv, win_send, win_recv, mate_send, mate_recv, res_send, res_recv, load_sem,
):
    local = 2 * bpb
    b = lax.axis_index("bunch")
    d = lax.axis_index("dom")
    beam = lax.div(d, bpb)
    member = lax.rem(d, bpb)
    source = lax.rem(d + bpb, local)
    pad = 2 * OFFSET
    rows = cells + pad

    def at(block, dom):
        return (block, dom)

    barrier = pltpu.get_barrier_semaphore()
    jumps = [j for h in range(1, HOPS + 1) for j in (h, -h)]
    for k in range(1, nd):
        pl.semaphore_signal(barrier, inc=1, device_id=at(b, lax.rem(d + k, nd)), device_id_type=MESH)
    for j in jumps:
        pl.semaphore_signal(barrier, inc=1, device_id=at(lax.rem(b + j + nb, nb), d), device_id_type=MESH)

    loads = [
        pltpu.make_async_copy(a, v, load_sem.at[i])
        for i, (a, v) in enumerate(
            [(t1_hbm, t1), (t2_hbm, t2), (kernel_hbm, kern), (t3_hbm, t3), (t4_hbm, t4)]
        )
    ]
    for load in loads:
        load.start()
    for e in range(2):
        for m in range(bpb):
            for c in range(2):
                pos_s[e * bpb + m, c : c + 1, :] = pos[c, e, m : m + 1, :]
    zero = jnp.zeros((2 * HOPS + 1, bpb, pad, cells), F32)
    win[:, :, :pad, :] = zero
    win[:, :, pad + cells :, :] = zero
    def fill(coords):
        for p in range(0, parts, LANES):
            sl = slice(p, p + LANES)
            high, low = hat_split(coords[0:1, sl], cells)
            tx[:cells, sl] = high
            tx[cells:, sl] = low
            high, low = hat_split(coords[1:2, sl], cells)
            ty[:cells, sl] = high
            ty[cells:, sl] = low
        return lax.dot_general(
            tx[...], ty[...], (((1,), (1,)), ((), ())), preferred_element_type=F32
        )

    def kick_tables(coords, base):
        for p in range(0, parts, LANES):
            sl = slice(p, p + LANES)
            to = slice(base + p, base + p + LANES)
            wx[:, to] = hat(coords[0:1, sl], cells)
            high, low = hat_split(coords[1:2, sl], cells)
            wy[:cells, to] = high
            wy[cells : 2 * cells, to] = high
            wy[2 * cells :, to] = low

    total = fill(pos_s[source])
    kick_tables(pos_s[d], 0)
    pl.semaphore_wait(barrier, nd - 1 + len(jumps))

    sends = []
    for which in range(2):
        for k in range(1, nd):
            peer = lax.rem(d + k, nd)
            bunch = lax.rem(peer + bpb, local) if which == 0 else peer
            copy = pltpu.make_async_remote_copy(
                src_ref=pos_s.at[bunch],
                dst_ref=rx.at[k - 1, which],
                send_sem=pos_send.at[k - 1, which],
                recv_sem=pos_recv.at[k - 1, which],
                device_id=at(b, peer),
                device_id_type=MESH,
            )
            copy.start()
            sends.append(copy)

    for k in range(1, nd):
        sends[k - 1].wait_recv()
        total = total + fill(rx[k - 1, 0])
    grid = (
        total[:cells, :cells] + total[:cells, cells:] + total[cells:, :cells] + total[cells:, cells:]
    )
    band = pl.ds(pad, cells)
    win[HOPS, member, band, :] = grid

    grid_sends = {}
    for i, j in enumerate(jumps):
        copy = pltpu.make_async_remote_copy(
            src_ref=win.at[HOPS, member, band],
            dst_ref=win.at[HOPS - j, member, band],
            send_sem=win_send.at[i],
            recv_sem=win_recv.at[i],
            device_id=at(lax.rem(b + j + nb, nb), d),
            device_id_type=MESH,
        )
        copy.start()
        grid_sends[j] = copy
    mate_sends = []

    def to_mates(place):
        for k in range(1, bpb):
            mate = beam * bpb + lax.rem(member + k, bpb)
            copy = pltpu.make_async_remote_copy(
                src_ref=win.at[place, member, band],
                dst_ref=win.at[place, member, band],
                send_sem=mate_send.at[place, k - 1],
                recv_sem=mate_recv.at[place, k - 1],
                device_id=at(b, mate),
                device_id_type=MESH,
            )
            copy.start()
            mate_sends.append((place, k, copy))

    to_mates(HOPS)

    for k in range(1, nd):
        sends[nd - 1 + k - 1].wait_recv()
        kick_tables(rx[k - 1, 1], k * parts)
    for j in jumps:
        grid_sends[j].wait_recv()
        to_mates(HOPS - j)
    for place, k, copy in mate_sends:
        copy.wait_recv()

    live_count = counts[beam, member]
    lane = lax.broadcasted_iota(jnp.int32, (8, cells), 1)
    chosen = []
    for s in range(slots):
        row = partners[beam, member, s]
        place = jnp.minimum(lax.rem(lax.div(row, bpb) - b + HOPS + nb, nb), 2 * HOPS)
        shift_x = offsets[0, beam, member, s]
        shift_y = offsets[1, beam, member, s]
        turn = jnp.where(shift_y < 0, shift_y + cells, shift_y)
        live = jnp.where(s < live_count, 1.0, 0.0).astype(F32)
        wrap = jnp.where(shift_y < 0, 1, 0)
        upper = jnp.where(lane >= turn, 1, 0)
        first = jnp.where(upper != wrap, live, 0.0)
        chosen.append((place, lax.rem(row, bpb), OFFSET - shift_x, turn, first, live - first))
    step = 2 * OFFSET
    for r in range(0, rows, step):
        low_half = jnp.zeros((step, cells), F32)
        high_half = jnp.zeros((step, cells), F32)
        for place, which, start, turn, first, second in chosen:
            piece = win[place, which, pl.ds(start + r, step), :]
            piece = pltpu.roll(piece, turn, 1)
            low_half = low_half + piece * jnp.concatenate([first] * (step // 8), 0)
            high_half = high_half + piece * jnp.concatenate([second] * (step // 8), 0)
        src[r : r + step, :cells] = low_half
        src[r : r + step, cells:] = high_half

    loads[0].wait()
    sh, sl = split(src[...])
    spec = dot3(t1[0], t1[1], sh, sl)
    real, imag = spec[:padded], spec[padded:]
    ah, al = split(real)
    bh, bl = split(imag)

    def pair(x, y):
        return jnp.concatenate(
            [jnp.concatenate([x, y], 1), jnp.concatenate([y, -x], 1)], 0
        )

    loads[1].wait()
    spec = dot3(pair(ah, bh), pair(al, bl), t2[0], t2[1])
    real, imag = spec[:padded], spec[padded:]
    loads[2].wait()
    mixed = []
    for c in range(2):
        kr, ki = kern[c, 0], kern[c, 1]
        mixed.append(jnp.concatenate([kr * real - ki * imag, kr * imag + ki * real], 1))
    mh, ml = split(jnp.concatenate(mixed, 0))
    loads[3].wait()
    half = dot3(mh, ml, t3[0], t3[1])
    g0, g1 = half[:padded], half[padded:]
    stacked = jnp.concatenate(
        [
            jnp.concatenate([g0[:, :cells], g1[:, :cells]], 1),
            jnp.concatenate([g0[:, cells:], g1[:, cells:]], 1),
        ],
        0,
    )
    gh, gl = split(stacked)
    loads[4].wait()
    field = dot3(t4[0], t4[1], gh, gl)
    fh, fl = split(jnp.concatenate([field[:, :cells], field[:, cells:]], 0))
    weights = jnp.concatenate([fh, fl, fh], 1)

    def kicks(k):
        for p in range(0, parts, LANES):
            sl = slice(k * parts + p, k * parts + p + LANES)
            z = dot(weights, wy[:, sl])
            w = wx[:, sl]
            for c in range(2):
                row = jnp.sum(z[c * cells : (c + 1) * cells] * w, axis=0, keepdims=True)
                res[k, c : c + 1, p : p + LANES] = row

    res_sends = []
    for k in range(1, nd):
        kicks(k)
        copy = pltpu.make_async_remote_copy(
            src_ref=res.at[k],
            dst_ref=fin.at[d],
            send_sem=res_send.at[k - 1],
            recv_sem=res_recv.at[k - 1],
            device_id=at(b, lax.rem(d - k + nd, nd)),
            device_id_type=MESH,
        )
        copy.start()
        res_sends.append(copy)
    kicks(0)
    fin[d] = res[0]
    for copy in res_sends:
        copy.wait_recv()
    for e in range(2):
        for m in range(bpb):
            for c in range(2):
                out[c, e, m : m + 1, :] = fin[e * bpb + m, c : c + 1, :]
    for copy in sends + list(grid_sends.values()) + res_sends:
        copy.wait_send()
    for _, _, copy in mate_sends:
        copy.wait_send()


def solution(mesh):
    nb, nd = mesh.shape["bunch"], mesh.shape["dom"]

    def per_device(positions, momenta, kernel_hat, partners, offsets, counts):
        bpb = positions.shape[2]
        parts = positions.shape[3]
        padded = kernel_hat.shape[-1]
        cells = padded // 2
        slots = partners.shape[-1]
        local = 2 * bpb
        assert local == nd and nb > 2 * HOPS
        pad = 2 * OFFSET
        rows = cells + pad
        tables = [jnp.asarray(t) for t in dft_tables(padded, cells, rows)]
        vmem = pl.BlockSpec(memory_space=pltpu.VMEM)
        smem = pl.BlockSpec(memory_space=pltpu.SMEM)
        anym = pl.BlockSpec(memory_space=pl.ANY)
        dma = pltpu.SemaphoreType.DMA
        kicks = pl.pallas_call(
            functools.partial(body, nb, nd, bpb, cells, padded, parts, slots),
            out_shape=jax.ShapeDtypeStruct(momenta.shape, F32),
            in_specs=[smem] * 3 + [vmem] + [anym] * 5,
            out_specs=vmem,
            scratch_shapes=[
                pltpu.VMEM((local, 2, parts), F32),
                pltpu.VMEM((nd - 1, 2, 2, parts), F32),
                pltpu.VMEM((2 * cells, parts), BF),
                pltpu.VMEM((2 * cells, parts), BF),
                pltpu.VMEM((2 * HOPS + 1, bpb, cells + 2 * pad, cells), F32),
                pltpu.VMEM((cells, nd * parts), F32),
                pltpu.VMEM((3 * cells, nd * parts), BF),
                pltpu.VMEM((rows, padded), F32),
                pltpu.VMEM((nd, 2, parts), F32),
                pltpu.VMEM((local, 2, parts), F32),
                pltpu.VMEM(kernel_hat.shape, F32),
            ]
            + [pltpu.VMEM(t.shape, BF) for t in tables]
            + [
                dma((nd - 1, 2)),
                dma((nd - 1, 2)),
                dma((2 * HOPS,)),
                dma((2 * HOPS,)),
                dma((2 * HOPS + 1, bpb - 1)),
                dma((2 * HOPS + 1, bpb - 1)),
                dma((nd - 1,)),
                dma((nd - 1,)),
                dma((5,)),
            ],
            compiler_params=pltpu.CompilerParams(collective_id=0, has_side_effects=True),
            name="beam_kick",
        )(partners, offsets, counts, positions, kernel_hat, *tables)
        return momenta + kicks

    spec = P(None, None, "bunch", "dom")
    return jax.shard_map(
        per_device,
        mesh=mesh,
        in_specs=(spec, spec, P(), P(None, "bunch", None), P(None, None, "bunch", None), P(None, "bunch")),
        out_specs=spec,
        check_vma=False,
    )
```
